32 devices in a mesh: section: 4 (over y, core), seq: 8 (over z, x).
Axes of the slice: x: 2, y: 2, z: 4, core: 2. Of those that a mesh axis runs over, the one named last changes fastest.
Arguments:
- queries: bfloat16 [4, 1024, 2048], P('section', 'seq'), may hold values from -4 to 4
- memory_keys: bfloat16 [4, 1024, 2048], P('section', 'seq'), may hold values from -2.5 to 2.5
- memory_values: bfloat16 [4, 1024, 2048], P('section', 'seq'), may hold values from -4 to 4
- upstream: bfloat16 [4, 1024, 2048], P('section', 'seq'), may hold values from -4 to 4
- inner_rate: float32 [4, 32], P('section'), may hold values from 0.02 to 0.2
- checkpoints: float32 [4, 8, 32, 4096], P('section', 'seq'), may hold values from -0.75 to 0.75
Outputs:
- grad_queries: bfloat16 [4, 1024, 2048], P('section', 'seq')
- grad_keys: bfloat16 [4, 1024, 2048], P('section', 'seq')
- grad_values: bfloat16 [4, 1024, 2048], P('section', 'seq')
- adjoint_start: float32 [4, 8, 32, 4096], P('section', 'seq')
The draws below stay inside these ranges and needn't reach their ends.
All inputs are finite; a program needn't handle non-finite values.
Results may differ from the reference program's by a relative error of at most 0.001.
Values may be sent and summed in bfloat16 or wider, within the bound.
A program may use at most 128 MiB of HBM per device.

```python
import math
from functools import partial
import jax
import jax.numpy as jnp
from jax import lax

H = 32
DH = 64
MB = 64
TOK_DEV = 128
SECTIONS = 4
SHARDS = 8
TOKENS = 1024
HD = 2048


def shard_levels(own_key, shape, shards, low, high):
    level = 1.0
    for position, shards_of in shards:
        draws = jax.random.uniform(jax.random.fold_in(jax.random.fold_in(own_key, 6), position), (shards_of,), jnp.float32, low / len(shards), high / len(shards))
        level = level * jnp.repeat(jnp.exp(draws), shape[position] // shards_of).reshape((-1,) + (1,) * (len(shape) - 1 - position))
    return level


def centred(key, dims, deviation, limit, cuts=(), kind=jnp.bfloat16):
    loudness = shard_levels(key, dims, cuts, -0.22, 0.18) if cuts else 1.0
    values = jax.random.normal(key, dims, jnp.float32) * deviation * loudness
    return jnp.minimum(jnp.maximum(values, -limit), limit).astype(kind)


def setup_inputs(seed: int = 0) -> dict:
    key_list = jax.random.split(jax.random.key(seed), 7)
    queries = centred(key_list[0], (SECTIONS, TOKENS, HD), 1.0, 4.0, ((0, 4), (1, 8)))
    memory_keys = centred(key_list[1], (SECTIONS, TOKENS, HD), 1.0, 2.5, ((0, 4), (1, 8)))
    memory_values = centred(key_list[2], (SECTIONS, TOKENS, HD), 1.0, 4.0, ((0, 4), (1, 8)))
    upstream = centred(key_list[3], (SECTIONS, TOKENS, HD), 1.0, 4.0, ((0, 4), (1, 8)))
    inner_rate = jnp.clip(jnp.exp(math.log(0.2) - 2.3025851 * jax.random.uniform(key_list[4], (SECTIONS, H), jnp.float32) ** shard_levels(key_list[4], (SECTIONS, H), ((0, 4),), -0.2, 0.2)), 0.02, 0.2)
    checkpoints = centred(key_list[5], (SECTIONS, SHARDS, H, DH * DH), DH ** -0.5, 0.75, ((0, 4), (1, 8)), jnp.float32)
    return {"queries": queries, "memory_keys": memory_keys, "memory_values": memory_values, "upstream": upstream, "inner_rate": inner_rate, "checkpoints": checkpoints}


inner_product = partial(jnp.einsum, precision=lax.Precision.HIGHEST)


def lower_mask():
    row_index = lax.broadcasted_iota(jnp.int32, (MB, MB), 0)
    col_index = lax.broadcasted_iota(jnp.int32, (MB, MB), 1)
    return (row_index >= col_index).astype(jnp.float32)


def to_blocks(array):
    shaped = array.astype(jnp.float32).reshape(TOKENS // MB, MB, H, DH)
    return jnp.transpose(shaped, (0, 2, 1, 3))


def from_blocks(array):
    return jnp.transpose(array, (0, 2, 1, 3)).reshape(TOKENS, H * DH).astype(jnp.bfloat16)


def shard_major(array):
    per_shard = TOK_DEV // MB
    shaped = array.reshape((SHARDS, per_shard) + array.shape[1:])
    return jnp.swapaxes(shaped, 0, 1)


def block_major(array):
    return jnp.swapaxes(array, 0, 1).reshape((TOKENS // MB,) + array.shape[2:])


def one_section(operands):
    queries, memory_keys, memory_values, cotangent, inner_rate, checkpoints = operands
    per_shard = TOK_DEV // MB
    update_rate = (inner_rate / MB)[:, None, None]
    masked_scores = lower_mask()
    query_blocks = to_blocks(queries)
    key_blocks = to_blocks(memory_keys)
    value_blocks = to_blocks(memory_values)
    grad_blocks = to_blocks(cotangent)
    initial = checkpoints.reshape(SHARDS, H, DH, DH)

    def forward(weight_stack, pieces):
        current_key, current_value = pieces
        error_rows = inner_product("shmd,shde->shme", current_key, weight_stack) - current_value
        updated_weight = weight_stack - update_rate * inner_product("shmd,shme->shde", current_key, error_rows)
        return updated_weight, (weight_stack, error_rows)

    trails = lax.scan(forward, initial, (shard_major(key_blocks), shard_major(value_blocks)))[1]
    weight_trail = block_major(trails[0])
    error_trail = block_major(trails[1])

    def backward(adjoint_carry, pieces):
        current_query, current_key, current_gradient, current_weight, error_now = pieces
        attention_scores = inner_product("sxi,sbi->sxb", current_query, current_key) * masked_scores
        error_gradient = -update_rate * (inner_product("hmn,hme->hne", attention_scores, current_gradient) + inner_product("hnd,hde->hne", current_key, adjoint_carry))
        score_gradient = -update_rate * inner_product("hme,hne->hmn", current_gradient, error_now) * masked_scores
        query_gradient = inner_product("nyv,nxv->nyx", current_gradient, current_weight) + inner_product("clo,coq->clq", score_gradient, current_key)
        grad_key = (inner_product("hne,hde->hnd", error_gradient, current_weight)
                    - update_rate * inner_product("hne,hde->hnd", error_now, adjoint_carry)
                    + inner_product("fbw,fbe->fwe", score_gradient, current_query))
        previous_weight = adjoint_carry + inner_product("fwl,fwn->fln", current_query, current_gradient) + inner_product("wik,wiy->wky", current_key, error_gradient)
        return previous_weight, (query_gradient, grad_key, -error_gradient, previous_weight)

    empty = jnp.zeros((H, DH, DH), jnp.float32)
    results = lax.scan(backward, empty, (query_blocks, key_blocks, grad_blocks, weight_trail, error_trail), reverse=True)[1]
    starts = results[3].reshape(SHARDS, per_shard, H, DH, DH)[:, 0].reshape(SHARDS, H, DH * DH)
    return from_blocks(results[0]), from_blocks(results[1]), from_blocks(results[2]), starts


def reference(queries, memory_keys, memory_values, upstream, inner_rate, checkpoints):
    cotangent = jnp.roll(upstream, -1, axis=0)
    grad_queries, grad_keys, grad_values, adjoint_start = lax.map(
        one_section, (queries, memory_keys, memory_values, cotangent, inner_rate, checkpoints))
    return grad_queries, grad_keys, grad_values, adjoint_start
```

```python
from functools import partial

import jax
import jax.numpy as jnp
from jax import lax
from jax.experimental import pallas as pl
from jax.experimental.pallas import tpu as pltpu
from jax.sharding import PartitionSpec as P

MB = 64
LANES = 128
F32 = jnp.float32
BF16 = jnp.bfloat16
MESH = pl.DeviceIdType.MESH


def nn(a, b):
    return lax.dot_general(a, b, (((1,), (0,)), ((), ())), preferred_element_type=F32)


def nt(a, b):
    return lax.dot_general(a, b, (((1,), (1,)), ((), ())), preferred_element_type=F32)


def tn(a, b):
    return lax.dot_general(a, b, (((0,), (0,)), ((), ())), preferred_element_type=F32)


def split(x):
    high = x.astype(BF16)
    return high, (x - high.astype(F32)).astype(BF16)


def stacked(parts):
    return jnp.concatenate(parts, axis=0)


def tiles(x):
    return [x[:, i : i + LANES] for i in range(0, x.shape[1], LANES)]


def diagonal(x, dh):
    per = LANES // dh
    lane = lax.broadcasted_iota(jnp.int32, (x.shape[0], LANES), 1) // dh
    masks = [(lane == i).astype(F32).astype(BF16) for i in range(per)]
    pieces = tiles(x)
    zero = jnp.zeros((x.shape[0], LANES), x.dtype)
    rows = []
    for t, piece in enumerate(pieces):
        for i in range(per):
            row = [zero] * len(pieces)
            row[t] = piece * masks[i]
            rows.append(jnp.concatenate(row, axis=1))
    return stacked(rows)


def folded(a, b, dh):
    per = LANES // dh
    lane = lax.broadcasted_iota(jnp.int32, (dh, LANES), 1) // dh
    out = []
    for left, right in zip(tiles(a), tiles(b)):
        product = tn(left, right)
        value = product[:dh]
        for i in range(1, per):
            value = jnp.where(lane == i, product[i * dh : (i + 1) * dh], value)
        out.append(value)
    return jnp.concatenate(out, axis=1)


def rows_times(x, weights, multiply=nn):
    high, low = split(x)
    both = multiply(stacked([high, low]), weights)
    return both[: x.shape[0]] + both[x.shape[0] :]


def full_times(x, weights, multiply=nn):
    return rows_times(x, weights[0], multiply) + multiply(x.astype(BF16), weights[1])


def halves(x, dh):
    high, low = split(x)
    return diagonal(high, dh), diagonal(low, dh)


def exact_times(x, weights, multiply=nn):
    return multiply(x, weights[0]) + multiply(x, weights[1])


def doubled(a, b):
    return stacked([a, a]), stacked(split(b))


def lane_index(shape, dh):
    return lax.broadcasted_iota(jnp.int32, shape, 1) % dh


def upper_mask(width):
    row = lax.broadcasted_iota(jnp.int32, (MB, width), 0)
    return (lane_index((MB, width), MB) >= row).astype(F32)


def weight_part(k, v, c, w, dh):
    weights, errors = [], []
    for t in range(len(k)):
        e = exact_times(k[t], halves(w, dh)) - v[t].astype(F32)
        yield
        weights.append(w)
        errors.append(e)
        if t + 1 < len(k):
            w = w - c * folded(*doubled(k[t], e), dh)
            yield
    return weights, errors


def linear_part(k, c, dh):
    width = c.shape[1]
    row = lax.broadcasted_iota(jnp.int32, (dh, width), 0)
    eye = jnp.where(row == lane_index((dh, width), dh), 1.0, 0.0)
    linear = []
    for block in k:
        linear.append(eye - c * folded(block, block, dh))
        yield
    a = linear[-1]
    for t in range(len(k) - 2, -1, -1):
        a = full_times(linear[t], halves(a, dh))
        yield
    return a


def pair_linear(near, far, is_even, c, dh):
    near_a = yield from linear_part(near, c, dh)
    far_a = yield from linear_part(far, c, dh)
    first = jnp.where(is_even, near_a, far_a)
    second = jnp.where(is_even, far_a, near_a)
    both = full_times(first, halves(second, dh))
    yield
    return first, second, both


def interleaved(runs):
    results, waiting = [None] * len(runs), dict(enumerate(runs))
    while waiting:
        for i, run in list(waiting.items()):
            try:
                next(run)
            except StopIteration as stop:
                results[i] = stop.value
                del waiting[i]
    return results


def step_back(q, k, z, error_grad, dh):
    high, low = split(error_grad)
    return folded(stacked([q, k, k]), stacked([z, high, low]), dh)


def source_part(q, k, z, c, dh):
    upper = upper_mask(c.shape[1])
    carried = [None] * len(k)
    for t in range(len(k) - 1, -1, -1):
        scores = nt(k[t], diagonal(q[t], dh)) * upper
        yield
        carried[t] = rows_times(scores, diagonal(z[t], dh))
        yield
    b = None
    for t in range(len(k) - 1, -1, -1):
        total = carried[t] if b is None else carried[t] + exact_times(k[t], halves(b, dh))
        yield
        update = step_back(q[t], k[t], z[t], total * -c, dh)
        b = update if b is None else b + update
        yield
    return carried, b


def score_part(q, k, z, c, weights, errors, dh):
    upper = upper_mask(c.shape[1])
    query_grads, key_part = [], []
    for t in range(len(k)):
        score_grad = rows_times(errors[t], diagonal(z[t], dh), nt) * (upper * -c)
        yield
        key_part.append(rows_times(score_grad, diagonal(q[t], dh)))
        yield
        high, low = split(score_grad)
        query_grads.append(
            exact_times(z[t], halves(weights[t], dh), nt)
            + folded(stacked([high, low]), stacked([k[t], k[t]]), dh)
        )
        yield
    return query_grads, key_part


def final_part(q, k, z, c, weights, errors, carried, key_part, g, dh):
    count = len(q)
    key_grads, value_grads = [None] * count, [None] * count
    for t in range(count - 1, -1, -1):
        whole = halves(g, dh)
        minus = c * (carried[t] + exact_times(k[t], whole))
        yield
        value_grads[t] = minus
        g = g + step_back(q[t], k[t], z[t], -minus, dh)
        yield
        partial_grad = key_part[t] - c * full_times(errors[t], whole, nt)
        yield
        key_grads[t] = partial_grad - full_times(minus, halves(weights[t], dh), nt)
        yield
    return key_grads, value_grads, g


def cut(ref, lanes, size=MB):
    return [ref[i : i + size, lanes] for i in range(0, ref.shape[0], size)]


def put(ref, lanes, parts):
    size = ref.shape[0] // len(parts)
    for i, part in enumerate(parts):
        ref[i * size : (i + 1) * size, lanes] = part.astype(ref.dtype)


def kernel(
    dh, unit, upstream, q_in, k_in, v_in, rates, checkpoint,
    gq, gk, gv, rows_of_heads,
    q, k, v, in_sems, stage,
    z, far_k, trail, err, car, kp, b, other_b, first_a, second_a, pair_a, pair_b, second_b,
    entering, leaving, back, end,
    line_sem, up_send, up_recv, k_send, k_recv, b_send, b_recv, g_send, g_recv, r_send, r_recv,
):
    shard, shards = lax.axis_index("seq"), lax.axis_size("seq")
    section, sections = lax.axis_index("section"), lax.axis_size("section")
    features = q.shape[1]
    half = features // 2
    units = half // unit
    piece = 2 * LANES
    pieces = half // piece
    per_unit = unit // piece
    fine = piece // LANES
    side = lax.rem(shard, 2)
    is_even = side == 0
    partner = (section, shard + 1 - 2 * side)
    before = (section, jnp.maximum(shard - 2, 0))
    after = (section, jnp.minimum(shard + 2, shards - 1))
    below = (lax.rem(section + sections - 1, sections), shard)
    above = (lax.rem(section + 1, sections), shard)
    not_first = shard >= 2
    not_last = shard < shards - 2
    heads = features // dh
    lines = dh * dh // LANES

    def line_in(i):
        return pltpu.make_async_copy(
            checkpoint.at[:, pl.ds(i * LANES, LANES)],
            rows_of_heads.at[pl.ds(i * heads, heads), :],
            line_sem.at[i],
        )

    loads = [
        pltpu.make_async_copy(x, y, in_sems.at[i])
        for i, (x, y) in enumerate(((k_in, k), (v_in, v), (q_in, q)))
    ]
    loads[0].start()
    for i in range(lines):
        line_in(i).start()
    loads[1].start()
    loads[2].start()

    barrier = pltpu.get_barrier_semaphore()
    for peer in (below, above, partner):
        pl.semaphore_signal(barrier, inc=1, device_id=peer, device_id_type=MESH)
    for present, peer in ((not_first, before), (not_last, after)):
        @pl.when(present)
        def _():
            pl.semaphore_signal(barrier, inc=1, device_id=peer, device_id_type=MESH)

    def remote(source, target, send, recv, peer):
        return pltpu.make_async_remote_copy(
            src_ref=source, dst_ref=target, send_sem=send, recv_sem=recv,
            device_id=peer, device_id_type=MESH,
        )

    left = lax.broadcasted_iota(jnp.int32, (lines, LANES), 1) < dh

    def swap(x):
        return jnp.concatenate([x[:, dh:], x[:, :dh]], axis=1)

    def head_of(lanes):
        return (lanes.start // LANES) * (LANES // dh)

    def rate_of(lanes):
        head = head_of(lanes)
        first = lax.broadcasted_iota(jnp.int32, (1, LANES), 1) < dh
        return jnp.where(first, rates[0, head], rates[0, head + 1]) / MB

    def load_weight(lanes):
        head = head_of(lanes)
        x = rows_of_heads[pl.ds(head, lines, stride=heads), :]
        y = rows_of_heads[pl.ds(head + 1, lines, stride=heads), :]
        base = head * (dh // 2)
        stage[pl.ds(base, lines, stride=2), :] = jnp.where(left, x, swap(y))
        stage[pl.ds(base + 1, lines, stride=2), :] = jnp.where(left, swap(x), y)
        trail[:dh, lanes] = stage[pl.ds(pl.multiple_of(base, dh), dh), :]

    def store_start(lanes, first):
        head = head_of(lanes)
        base = head * (dh // 2)
        stage[pl.ds(pl.multiple_of(base, dh), dh), :] = first
        even = stage[pl.ds(base, lines, stride=2), :]
        odd = stage[pl.ds(base + 1, lines, stride=2), :]
        rows_of_heads[pl.ds(head, lines, stride=heads), :] = jnp.where(left, even, swap(odd))
        rows_of_heads[pl.ds(head + 1, lines, stride=heads), :] = jnp.where(left, swap(even), odd)

    def span(start, size):
        return pl.ds(pl.multiple_of(start, size), size)

    def own(i, size):
        return span(side * half + i * size, size)

    def others(i, size):
        return span((1 - side) * half + i * size, size)

    def place(i, size):
        return span(i * size, size)

    def send_up(i):
        lanes = span(lax.rem(1 - side + i // pieces, 2) * half + lax.rem(i, pieces) * piece, piece)
        return remote(upstream.at[:, lanes], z.at[:, lanes], up_send.at[i], up_recv.at[i], below)

    def send_k(i):
        return remote(
            k_in.at[:, others(i, piece)], far_k.at[:, place(i, piece)], k_send.at[i], k_recv.at[i], partner
        )

    def send_b(i):
        return remote(
            b.at[:, others(i, piece)], other_b.at[:, place(i, piece)], b_send.at[i], b_recv.at[i], partner
        )

    def send_g(i):
        return remote(
            leaving.at[:, place(i, LANES)], entering.at[:, place(i, LANES)], g_send.at[i], g_recv.at[i], before
        )

    def send_r(i):
        return remote(
            back.at[:, place(i, LANES)], end.at[:, own(i, LANES)], r_send.at[i], r_recv.at[i], partner
        )

    def await_r(i):
        return remote(
            back.at[:, place(i, LANES)], end.at[:, others(i, LANES)], r_send.at[i], r_recv.at[i], partner
        )

    def narrow(lanes):
        return [
            pl.ds(pl.multiple_of(lanes.start + j, LANES), LANES) for j in range(0, lanes.size, LANES)
        ]

    def together(compute, store, lanes):
        groups = narrow(lanes)
        results = interleaved([compute(x) for x in groups])
        for x, result in zip(groups, results):
            store(x, *result)

    def weights_of(lanes):
        return weight_part(cut(k, lanes), cut(v, lanes), rate_of(lanes), trail[:dh, lanes], dh)

    def put_weights(lanes, weights, errors):
        for t in range(1, len(weights)):
            trail[t * dh : (t + 1) * dh, lanes] = weights[t]
        put(err, lanes, errors)

    def sources_of(lanes):
        return source_part(cut(q, lanes), cut(k, lanes), cut(z, lanes), rate_of(lanes), dh)

    def put_sources(lanes, carried, offset):
        put(car, lanes, carried)
        b[:, lanes] = offset

    def scores_of(lanes):
        return score_part(
            cut(q, lanes), cut(k, lanes), cut(z, lanes), rate_of(lanes),
            cut(trail, lanes, dh), cut(err, lanes), dh,
        )

    def put_scores(lanes, query_grads, key_part):
        put(gq, lanes, query_grads)
        put(kp, lanes, key_part)

    def finals_of(lanes):
        return final_part(
            cut(q, lanes), cut(k, lanes), cut(z, lanes), rate_of(lanes),
            cut(trail, lanes, dh), cut(err, lanes), cut(car, lanes), cut(kp, lanes), end[:, lanes], dh,
        )

    def put_finals(lanes, key_grads, value_grads, first):
        put(gk, lanes, key_grads)
        put(gv, lanes, value_grads)
        store_start(lanes, first)

    def each(body, first, last):
        def step(i, nothing):
            body(i)
            return nothing

        lax.fori_loop(first, last, step, jnp.int32(0))

    def weight_step(i):
        lanes = span(i * unit, unit)
        for x in narrow(lanes):
            load_weight(x)
        together(weights_of, put_weights, lanes)

    def linear_step(i):
        for j in range(per_unit):
            send_k(i * per_unit + j).wait_recv()
        lanes = own(i, unit)
        offset = side * half

        def compute(x):
            local = pl.ds(pl.multiple_of(x.start - offset, LANES), LANES)
            return pair_linear(cut(k, x), cut(far_k, local), is_even, rate_of(x), dh)

        def store(x, first, second, both):
            local = pl.ds(pl.multiple_of(x.start - offset, LANES), LANES)
            first_a[:, local] = first
            second_a[:, local] = second
            pair_a[:, local] = both

        together(compute, store, lanes)

    def source_step(i):
        for j in range(per_unit):
            send_up(i * per_unit + j).wait_recv()
        lanes = span(lax.rem(1 - side + i // units, 2) * half + lax.rem(i, units) * unit, unit)
        together(sources_of, put_sources, lanes)

        @pl.when(i < units)
        def _():
            for j in range(per_unit):
                send_b(i * per_unit + j).start()

        @pl.when((i >= units - 1) & (i < 2 * units - 1))
        def _():
            linear_step(i - (units - 1))

    def pair_step(i):
        lanes, local = own(i, piece), place(i, piece)
        send_b(i).wait_recv()
        near_b, far_b = b[:, lanes], other_b[:, local]
        b1 = jnp.where(is_even, far_b, near_b)
        b0 = jnp.where(is_even, near_b, far_b)
        offset = full_times(first_a[:, local], halves(b1, dh)) + b0
        pair_b[:, local] = offset
        second_b[:, local] = b1

        @pl.when(not_first & jnp.logical_not(not_last))
        def _():
            leaving[:, local] = offset
            for j in range(fine):
                send_g(i * fine + j).start()

    sends_back = not_last | jnp.logical_not(is_even)
    gets_back = not_last | is_even

    def relay_step(i):
        lanes, local = own(i, LANES), place(i, LANES)

        @pl.when(not_last)
        def _():
            send_g(i).wait_recv()
            incoming = entering[:, local]
            whole = halves(incoming, dh)

            @pl.when(not_first)
            def _():
                leaving[:, local] = full_times(pair_a[:, local], whole) + pair_b[:, local]
                send_g(i).start()

            middle = full_times(second_a[:, local], whole) + second_b[:, local]
            back[:, local] = jnp.where(is_even, incoming, middle)
            end[:, lanes] = jnp.where(is_even, middle, incoming)

        @pl.when(jnp.logical_not(not_last))
        def _():
            middle = second_b[:, local]
            nothing = jnp.zeros_like(middle)
            end[:, lanes] = jnp.where(is_even, middle, nothing)

            @pl.when(jnp.logical_not(is_even))
            def _():
                back[:, local] = middle
                end[:, others(i, LANES)] = nothing

        @pl.when(sends_back)
        def _():
            send_r(i).start()

    def lanes_of(i):
        return span(lax.rem(side + i, 2) * half + (i // 2) * unit, unit)

    def score_step(i):
        together(scores_of, put_scores, lanes_of(i))

    def last_step(i):
        @pl.when((lax.rem(i, 2) == 1) & gets_back)
        def _():
            for j in range(unit // LANES):
                await_r((i // 2) * (unit // LANES) + j).wait_recv()

        together(finals_of, put_finals, lanes_of(i))

    for i in range(lines):
        line_in(i).wait()
    loads[0].wait()
    loads[1].wait()
    each(weight_step, 0, 1)
    pl.semaphore_wait(barrier, 3 + not_first.astype(jnp.int32) + not_last.astype(jnp.int32))
    for i in range(pieces):
        send_up(i).start()
        send_k(i).start()
    for i in range(pieces, 2 * pieces):
        send_up(i).start()
    each(weight_step, 1, 2 * units)
    loads[2].wait()
    each(source_step, 0, 2 * units)

    distance = (shards - 1 - shard) // 2
    relay_at = jnp.where(distance == 0, 0, jnp.where(distance == 1, pieces - 1, pieces + 1))
    early = jnp.where(not_first, 0, 1)
    total = 2 * units

    def slot(n):
        @pl.when(n < pieces)
        def _():
            pair_step(n)

        @pl.when((n >= relay_at) & (n < relay_at + pieces))
        def _():
            for j in range(fine):
                relay_step((n - relay_at) * fine + j)

        @pl.when((n >= 1) & (n <= total))
        def _():
            score_step(n - 1)

        now = n - relay_at
        index = jnp.where((early == 1) & (now == 1), 0, now - 3 + early)

        @pl.when((index >= early * (now >= 3).astype(jnp.int32)) & (index < total) & ((now >= 3) | (early == 1)) & (now != 2) & (now >= 1))
        def _():
            last_step(index)

    each(slot, 0, relay_at + 3 + total)

    def drain(i):
        send_k(i).wait_send()
        send_b(i).wait_send()
        for j in range(2):
            send_up(i * 2 + j).wait_send()
        for j in range(fine):
            @pl.when(sends_back)
            def _():
                send_r(i * fine + j).wait_send()

            @pl.when(not_first)
            def _():
                send_g(i * fine + j).wait_send()

    each(drain, 0, pieces)


def store_kernel(heads, gq, gk, gv, rows, gq_out, gk_out, gv_out, start_out, sems, line_sem):
    copies = [
        pltpu.make_async_copy(
            rows.at[pl.ds(i * heads, heads), :], start_out.at[:, pl.ds(i * LANES, LANES)], line_sem.at[i]
        )
        for i in range(rows.shape[0] // heads)
    ] + [
        pltpu.make_async_copy(x, y, sems.at[i])
        for i, (x, y) in enumerate(((gq, gq_out), (gk, gk_out), (gv, gv_out)))
    ]
    for copy in copies:
        copy.start()
    for copy in copies:
        copy.wait()


def per_device(queries, memory_keys, memory_values, upstream, inner_rate, checkpoints):
    heads = inner_rate.shape[1]
    features = queries.shape[2]
    dh = features // heads
    tokens = queries.shape[1]
    half = features // 2
    unit = min(4 * LANES, half)
    pieces = half // (2 * LANES)
    count = tokens // MB

    vmem = pl.BlockSpec(memory_space=pltpu.VMEM)
    hbm = pl.BlockSpec(memory_space=pl.ANY)
    kept = pl.BlockSpec(memory_space=pltpu.HBM)
    assert 2 * dh == LANES
    lines = dh * dh // LANES
    tall = jax.ShapeDtypeStruct((tokens, features), BF16)
    held = pltpu.VMEM((tokens, features), BF16)
    whole = pltpu.VMEM((dh, features), F32)
    part = pltpu.VMEM((dh, half), F32)
    rows = pltpu.VMEM((tokens, features), F32)
    gq, gk, gv, start_rows = pl.pallas_call(
        partial(kernel, dh, unit),
        in_specs=[kept] * 4 + [pl.BlockSpec(memory_space=pltpu.SMEM), kept],
        out_specs=[vmem] * 4,
        out_shape=[held, held, held, pltpu.VMEM((lines * heads, LANES), F32)],
        scratch_shapes=[held, held, held, pltpu.SemaphoreType.DMA((3,))] + [
            pltpu.VMEM((features // LANES * dh, LANES), F32),
            held,
            pltpu.VMEM((tokens, half), BF16),
            pltpu.VMEM((count * dh, features), F32),
            rows, rows, rows,
            whole,
            part, part, part, part, part, part,
            part, part, part,
            whole,
            pltpu.SemaphoreType.DMA((lines,)),
        ] + [pltpu.SemaphoreType.DMA((2 * pieces,))] * 2
        + [pltpu.SemaphoreType.DMA((pieces,))] * 4
        + [pltpu.SemaphoreType.DMA((half // LANES,))] * 4,
        compiler_params=pltpu.CompilerParams(collective_id=0, has_side_effects=True, vmem_limit_bytes=61 * 2**20 + 2**19),
        name="layer_backward",
    )(upstream[0], queries[0], memory_keys[0], memory_values[0], inner_rate, checkpoints[0, 0])
    gq, gk, gv, start = pl.pallas_call(
        partial(store_kernel, heads),
        in_specs=[hbm] * 4,
        out_specs=[hbm] * 4,
        out_shape=[tall, tall, tall, jax.ShapeDtypeStruct((heads, dh * dh), F32)],
        scratch_shapes=[pltpu.SemaphoreType.DMA((3,)), pltpu.SemaphoreType.DMA((lines,))],
        compiler_params=pltpu.CompilerParams(vmem_limit_bytes=2**20),
        name="store_results",
    )(gq, gk, gv, start_rows)
    return gq[None], gk[None], gv[None], start[None, None]


def solution(mesh):
    return jax.shard_map(
        per_device,
        mesh=mesh,
        in_specs=(
            P("section", "seq", None),
            P("section", "seq", None),
            P("section", "seq", None),
            P("section", "seq", None),
            P("section", None),
            P("section", "seq", None, None),
        ),
        out_specs=(
            P("section", "seq", None),
            P("section", "seq", None),
            P("section", "seq", None),
            P("section", "seq", None, None),
        ),
        check_vma=False,
    )
```

```python
from functools import partial

import jax
import jax.numpy as jnp
from jax import lax
from jax.experimental import pallas as pl
from jax.experimental.pallas import tpu as pltpu
from jax.sharding import PartitionSpec as P

MB = 64
LANES = 128
F32 = jnp.float32
BF16 = jnp.bfloat16
MESH = pl.DeviceIdType.MESH


def nn(a, b):
    return lax.dot_general(a, b, (((1,), (0,)), ((), ())), preferred_element_type=F32)


def nt(a, b):
    return lax.dot_general(a, b, (((1,), (1,)), ((), ())), preferred_element_type=F32)


def tn(a, b):
    return lax.dot_general(a, b, (((0,), (0,)), ((), ())), preferred_element_type=F32)


def split(x):
    high = x.astype(BF16)
    return high, (x - high.astype(F32)).astype(BF16)


def stacked(parts):
    return jnp.concatenate(parts, axis=0)


def tiles(x):
    return [x[:, i : i + LANES] for i in range(0, x.shape[1], LANES)]


def diagonal(x, dh):
    per = LANES // dh
    lane = lax.broadcasted_iota(jnp.int32, (x.shape[0], LANES), 1) // dh
    masks = [(lane == i).astype(F32).astype(BF16) for i in range(per)]
    pieces = tiles(x)
    zero = jnp.zeros((x.shape[0], LANES), x.dtype)
    rows = []
    for t, piece in enumerate(pieces):
        for i in range(per):
            row = [zero] * len(pieces)
            row[t] = piece * masks[i]
            rows.append(jnp.concatenate(row, axis=1))
    return stacked(rows)


def folded(a, b, dh):
    per = LANES // dh
    lane = lax.broadcasted_iota(jnp.int32, (dh, LANES), 1) // dh
    out = []
    for left, right in zip(tiles(a), tiles(b)):
        product = tn(left, right)
        value = product[:dh]
        for i in range(1, per):
            value = jnp.where(lane == i, product[i * dh : (i + 1) * dh], value)
        out.append(value)
    return jnp.concatenate(out, axis=1)


def rows_times(x, weights, multiply=nn):
    high, low = split(x)
    both = multiply(stacked([high, low]), weights)
    return both[: x.shape[0]] + both[x.shape[0] :]


def full_times(x, weights, multiply=nn):
    return rows_times(x, weights[0], multiply) + multiply(x.astype(BF16), weights[1])


def halves(x, dh):
    high, low = split(x)
    return diagonal(high, dh), diagonal(low, dh)


def exact_times(x, weights, multiply=nn):
    return multiply(x, weights[0]) + multiply(x, weights[1])


def doubled(a, b):
    return stacked([a, a]), stacked(split(b))


def lane_index(shape, dh):
    return lax.broadcasted_iota(jnp.int32, shape, 1) % dh


def upper_mask(width):
    row = lax.broadcasted_iota(jnp.int32, (MB, width), 0)
    return (lane_index((MB, width), MB) >= row).astype(F32)


def weight_part(k, v, c, w, dh):
    weights, errors = [], []
    for t in range(len(k)):
        e = exact_times(k[t], halves(w, dh)) - v[t].astype(F32)
        yield
        weights.append(w)
        errors.append(e)
        if t + 1 < len(k):
            w = w - c * folded(*doubled(k[t], e), dh)
            yield
    return weights, errors


def linear_part(k, c, dh):
    width = c.shape[1]
    row = lax.broadcasted_iota(jnp.int32, (dh, width), 0)
    eye = jnp.where(row == lane_index((dh, width), dh), 1.0, 0.0)
    linear = []
    for block in k:
        linear.append(eye - c * folded(block, block, dh))
        yield
    a = linear[-1]
    for t in range(len(k) - 2, -1, -1):
        a = full_times(linear[t], halves(a, dh))
        yield
    return a


def pair_linear(near, far, is_even, c, dh):
    near_a = yield from linear_part(near, c, dh)
    far_a = yield from linear_part(far, c, dh)
    first = jnp.where(is_even, near_a, far_a)
    second = jnp.where(is_even, far_a, near_a)
    both = full_times(first, halves(second, dh))
    yield
    return first, second, both


def interleaved(runs):
    results, waiting = [None] * len(runs), dict(enumerate(runs))
    while waiting:
        for i, run in list(waiting.items()):
            try:
                next(run)
            except StopIteration as stop:
                results[i] = stop.value
                del waiting[i]
    return results


def step_back(q, k, z, error_grad, dh):
    high, low = split(error_grad)
    return folded(stacked([q, k, k]), stacked([z, high, low]), dh)


def source_part(q, k, z, c, dh):
    upper = upper_mask(c.shape[1])
    carried = [None] * len(k)
    for t in range(len(k) - 1, -1, -1):
        scores = nt(k[t], diagonal(q[t], dh)) * upper
        yield
        carried[t] = rows_times(scores, diagonal(z[t], dh))
        yield
    b = None
    for t in range(len(k) - 1, -1, -1):
        total = carried[t] if b is None else carried[t] + exact_times(k[t], halves(b, dh))
        yield
        update = step_back(q[t], k[t], z[t], total * -c, dh)
        b = update if b is None else b + update
        yield
    return carried, b


def score_part(q, k, z, c, weights, errors, dh):
    upper = upper_mask(c.shape[1])
    query_grads, key_part = [], []
    for t in range(len(k)):
        score_grad = rows_times(errors[t], diagonal(z[t], dh), nt) * (upper * -c)
        yield
        key_part.append(rows_times(score_grad, diagonal(q[t], dh)))
        yield
        high, low = split(score_grad)
        query_grads.append(
            exact_times(z[t], halves(weights[t], dh), nt)
            + folded(stacked([high, low]), stacked([k[t], k[t]]), dh)
        )
        yield
    return query_grads, key_part


def final_part(q, k, z, c, weights, errors, carried, key_part, g, dh):
    count = len(q)
    key_grads, value_grads = [None] * count, [None] * count
    for t in range(count - 1, -1, -1):
        whole = halves(g, dh)
        minus = c * (carried[t] + exact_times(k[t], whole))
        yield
        value_grads[t] = minus
        g = g + step_back(q[t], k[t], z[t], -minus, dh)
        yield
        partial_grad = key_part[t] - c * full_times(errors[t], whole, nt)
        yield
        key_grads[t] = partial_grad - full_times(minus, halves(weights[t], dh), nt)
        yield
    return key_grads, value_grads, g


def cut(ref, lanes, size=MB):
    return [ref[i : i + size, lanes] for i in range(0, ref.shape[0], size)]


def put(ref, lanes, parts):
    size = ref.shape[0] // len(parts)
    for i, part in enumerate(parts):
        ref[i * size : (i + 1) * size, lanes] = part.astype(ref.dtype)


def kernel(
    dh, unit, upstream, q_in, k_in, v_in, rates, checkpoint,
    gq, gk, gv, rows_of_heads,
    q, k, v, in_sems, stage,
    z, far_k, trail, err, car, kp, b, other_b, first_a, second_a, pair_a, pair_b, second_b,
    entering, leaving, back, end,
    line_sem, up_send, up_recv, k_send, k_recv, b_send, b_recv, g_send, g_recv, r_send, r_recv,
):
    shard, shards = lax.axis_index("seq"), lax.axis_size("seq")
    section, sections = lax.axis_index("section"), lax.axis_size("section")
    features = q.shape[1]
    half = features // 2
    units = half // unit
    piece = 2 * LANES
    pieces = half // piece
    per_unit = unit // piece
    fine = piece // LANES
    side = lax.rem(shard, 2)
    is_even = side == 0
    partner = (section, shard + 1 - 2 * side)
    before = (section, jnp.maximum(shard - 2, 0))
    after = (section, jnp.minimum(shard + 2, shards - 1))
    below = (lax.rem(section + sections - 1, sections), shard)
    above = (lax.rem(section + 1, sections), shard)
    not_first = shard >= 2
    not_last = shard < shards - 2
    heads = features // dh
    lines = dh * dh // LANES

    def line_in(i):
        return pltpu.make_async_copy(
            checkpoint.at[:, pl.ds(i * LANES, LANES)],
            rows_of_heads.at[pl.ds(i * heads, heads), :],
            line_sem,
        )

    loads = [
        pltpu.make_async_copy(x, y, in_sems.at[i])
        for i, (x, y) in enumerate(((k_in, k), (v_in, v), (q_in, q)))
    ]
    loads[0].start()
    for i in range(lines):
        line_in(i).start()
    loads[1].start()
    loads[2].start()

    barrier = pltpu.get_barrier_semaphore()
    for peer in (below, above, partner):
        pl.semaphore_signal(barrier, inc=1, device_id=peer, device_id_type=MESH)
    for present, peer in ((not_first, before), (not_last, after)):
        @pl.when(present)
        def _():
            pl.semaphore_signal(barrier, inc=1, device_id=peer, device_id_type=MESH)

    def remote(source, target, send, recv, peer):
        return pltpu.make_async_remote_copy(
            src_ref=source, dst_ref=target, send_sem=send, recv_sem=recv,
            device_id=peer, device_id_type=MESH,
        )

    left = lax.broadcasted_iota(jnp.int32, (lines, LANES), 1) < dh

    def swap(x):
        return jnp.concatenate([x[:, dh:], x[:, :dh]], axis=1)

    def head_of(lanes):
        return (lanes.start // LANES) * (LANES // dh)

    def rate_of(lanes):
        head = head_of(lanes)
        first = lax.broadcasted_iota(jnp.int32, (1, LANES), 1) < dh
        return jnp.where(first, rates[0, head], rates[0, head + 1]) / MB

    def load_weight(lanes):
        head = head_of(lanes)
        x = rows_of_heads[pl.ds(head, lines, stride=heads), :]
        y = rows_of_heads[pl.ds(head + 1, lines, stride=heads), :]
        base = head * (dh // 2)
        stage[pl.ds(base, lines, stride=2), :] = jnp.where(left, x, swap(y))
        stage[pl.ds(base + 1, lines, stride=2), :] = jnp.where(left, swap(x), y)
        trail[:dh, lanes] = stage[pl.ds(pl.multiple_of(base, dh), dh), :]

    def store_start(lanes, first):
        head = head_of(lanes)
        base = head * (dh // 2)
        stage[pl.ds(pl.multiple_of(base, dh), dh), :] = first
        even = stage[pl.ds(base, lines, stride=2), :]
        odd = stage[pl.ds(base + 1, lines, stride=2), :]
        rows_of_heads[pl.ds(head, lines, stride=heads), :] = jnp.where(left, even, swap(odd))
        rows_of_heads[pl.ds(head + 1, lines, stride=heads), :] = jnp.where(left, swap(even), odd)

    def span(start, size):
        return pl.ds(pl.multiple_of(start, size), size)

    def own(i, size):
        return span(side * half + i * size, size)

    def others(i, size):
        return span((1 - side) * half + i * size, size)

    def place(i, size):
        return span(i * size, size)

    def source_lanes(i):
        return span(lax.rem(1 - side + i, 2) * half + (i // 2) * unit, unit)

    def send_up(i):
        start = source_lanes(i // per_unit).start + lax.rem(i, per_unit) * piece
        lanes = span(start, piece)
        return remote(upstream.at[:, lanes], z.at[:, lanes], up_send, up_recv.at[i], below)

    def send_k(i):
        return remote(
            k_in.at[:, others(i, piece)], far_k.at[:, place(i, piece)], k_send, k_recv.at[i], partner
        )

    def send_b(i):
        return remote(
            b.at[:, others(i, piece)], other_b.at[:, place(i, piece)], b_send, b_recv.at[i], partner
        )

    def send_g(i):
        return remote(
            leaving.at[:, place(i, LANES)], entering.at[:, place(i, LANES)], g_send, g_recv.at[i], before
        )

    def send_r(i, source):
        return remote(
            source.at[:, place(i, LANES)], end.at[:, own(i, LANES)], r_send, r_recv.at[i], partner
        )

    def await_r(i):
        return remote(
            back.at[:, place(i, LANES)], end.at[:, others(i, LANES)], r_send, r_recv.at[i], partner
        )

    sends_k = not_last | is_even
    gets_k = not_last | jnp.logical_not(is_even)
    sends_back = not_last | jnp.logical_not(is_even)
    gets_back = not_last | is_even

    def narrow(lanes):
        return [
            pl.ds(pl.multiple_of(lanes.start + j, LANES), LANES) for j in range(0, lanes.size, LANES)
        ]

    def together(compute, store, lanes):
        groups = narrow(lanes)
        results = interleaved([compute(x) for x in groups])
        for x, result in zip(groups, results):
            store(x, *result)

    def weights_of(lanes):
        return weight_part(cut(k, lanes), cut(v, lanes), rate_of(lanes), trail[:dh, lanes], dh)

    def put_weights(lanes, weights, errors):
        for t in range(1, len(weights)):
            trail[t * dh : (t + 1) * dh, lanes] = weights[t]
        put(err, lanes, errors)

    def sources_of(lanes):
        return source_part(cut(q, lanes), cut(k, lanes), cut(z, lanes), rate_of(lanes), dh)

    def put_sources(lanes, carried, offset):
        put(car, lanes, carried)
        b[:, lanes] = offset

    def scores_of(lanes):
        return score_part(
            cut(q, lanes), cut(k, lanes), cut(z, lanes), rate_of(lanes),
            cut(trail, lanes, dh), cut(err, lanes), dh,
        )

    def put_scores(lanes, query_grads, key_part):
        put(gq, lanes, query_grads)
        put(kp, lanes, key_part)

    def finals_of(lanes):
        return final_part(
            cut(q, lanes), cut(k, lanes), cut(z, lanes), rate_of(lanes),
            cut(trail, lanes, dh), cut(err, lanes), cut(car, lanes), cut(kp, lanes), end[:, lanes], dh,
        )

    def put_finals(lanes, key_grads, value_grads, first):
        put(gk, lanes, key_grads)
        put(gv, lanes, value_grads)
        store_start(lanes, first)

    def each(body, first, last):
        def step(i, nothing):
            body(i)
            return nothing

        lax.fori_loop(first, last, step, jnp.int32(0))

    def weight_step(i):
        lanes = span(i * unit, unit)
        for x in narrow(lanes):
            load_weight(x)
        together(weights_of, put_weights, lanes)

    def linear_step(i):
        @pl.when(gets_k)
        def _():
            for j in range(per_unit):
                send_k(i * per_unit + j).wait_recv()

        lanes = own(i, unit)
        offset = side * half

        def compute(x):
            local = pl.ds(pl.multiple_of(x.start - offset, LANES), LANES)
            return pair_linear(cut(k, x), cut(far_k, local), is_even, rate_of(x), dh)

        def store(x, first, second, both):
            local = pl.ds(pl.multiple_of(x.start - offset, LANES), LANES)
            first_a[:, local] = first
            second_a[:, local] = second
            pair_a[:, local] = both

        together(compute, store, lanes)

    def source_step(i):
        for j in range(per_unit):
            send_up(i * per_unit + j).wait_recv()
        together(sources_of, put_sources, source_lanes(i))

    def pair_step(i):
        lanes, local = own(i, piece), place(i, piece)
        send_b(i).wait_recv()
        near_b, far_b = b[:, lanes], other_b[:, local]
        b1 = jnp.where(is_even, far_b, near_b)
        b0 = jnp.where(is_even, near_b, far_b)
        offset = full_times(first_a[:, local], halves(b1, dh)) + b0
        pair_b[:, local] = offset
        second_b[:, local] = b1

        @pl.when(not_first & jnp.logical_not(not_last))
        def _():
            leaving[:, local] = offset
            for j in range(fine):
                send_g(i * fine + j).start()

    def relay_step(i):
        lanes, local = own(i, LANES), place(i, LANES)

        @pl.when(not_last)
        def _():
            send_g(i).wait_recv()

            @pl.when(is_even)
            def _():
                send_r(i, entering).start()

            incoming = entering[:, local]
            whole = halves(incoming, dh)

            @pl.when(not_first)
            def _():
                leaving[:, local] = full_times(pair_a[:, local], whole) + pair_b[:, local]
                send_g(i).start()

            middle = full_times(second_a[:, local], whole) + second_b[:, local]
            end[:, lanes] = jnp.where(is_even, middle, incoming)

            @pl.when(jnp.logical_not(is_even))
            def _():
                back[:, local] = middle
                send_r(i, back).start()

        @pl.when(jnp.logical_not(not_last))
        def _():
            middle = second_b[:, local]
            nothing = jnp.zeros_like(middle)
            end[:, lanes] = jnp.where(is_even, middle, nothing)

            @pl.when(jnp.logical_not(is_even))
            def _():
                back[:, local] = middle
                end[:, others(i, LANES)] = nothing
                send_r(i, back).start()

    def lanes_of(i):
        return span(lax.rem(side + i, 2) * half + (i // 2) * unit, unit)

    def score_step(i):
        together(scores_of, put_scores, lanes_of(i))

    def last_step(i):
        @pl.when((lax.rem(i, 2) == 1) & gets_back)
        def _():
            for j in range(unit // LANES):
                await_r((i // 2) * (unit // LANES) + j).wait_recv()

        together(finals_of, put_finals, lanes_of(i))

    pl.semaphore_wait(barrier, 3 + not_first.astype(jnp.int32) + not_last.astype(jnp.int32))
    for i in range(2 * pieces):
        send_up(i).start()

    @pl.when(sends_k)
    def _():
        for i in range(pieces):
            send_k(i).start()

    pltpu.make_async_copy(rows_of_heads, rows_of_heads, line_sem).wait()
    loads[0].wait()
    loads[1].wait()
    each(weight_step, 0, 2 * units)
    loads[2].wait()
    total = 2 * units

    def advance(n):
        even_slot = lax.rem(n, 2) == 0

        @pl.when(n < total)
        def _():
            source_step(n)

        @pl.when(even_slot & (n < total))
        def _():
            for j in range(per_unit):
                send_b((n // 2) * per_unit + j).start()

        @pl.when(even_slot & (n >= 2))
        def _():
            for j in range(per_unit):
                pair_step((n // 2 - 1) * per_unit + j)

        @pl.when(even_slot & (n < total))
        def _():
            linear_step(n // 2)

    each(advance, 0, total + 1)

    distance = (shards - 1 - shard) // 2
    near = distance == 1
    relay_at = jnp.where(distance == 0, 0, jnp.where(near, 1, total))
    early = jnp.where(not_first, 0, 1)

    def slot(n):
        now = n - relay_at

        @pl.when((now >= 0) & (now < pieces))
        def _():
            for j in range(fine):
                relay_step(now * fine + j)

        chosen = jnp.where(near, (n + 1) // 2, n)

        @pl.when((chosen < total) & (jnp.logical_not(near) | ((n != 1) & (n != 3))))
        def _():
            score_step(chosen)

        index = jnp.where(now == 1, 0, now - 3 + early)

        @pl.when((index < total) & ((now >= 3) | ((now == 1) & (early == 1))))
        def _():
            last_step(index)

    each(slot, 0, relay_at + 3 + total)

    remote(upstream, z, up_send, up_recv.at[0], below).wait_send()
    remote(b.at[:, others(0, half)], other_b, b_send, b_recv.at[0], partner).wait_send()

    @pl.when(sends_k)
    def _():
        remote(k_in.at[:, others(0, half)], far_k, k_send, k_recv.at[0], partner).wait_send()

    @pl.when(sends_back)
    def _():
        remote(back, end.at[:, own(0, half)], r_send, r_recv.at[0], partner).wait_send()

    @pl.when(not_first)
    def _():
        remote(leaving, entering, g_send, g_recv.at[0], before).wait_send()


def store_kernel(heads, gq, gk, gv, rows, gq_out, gk_out, gv_out, start_out, sems, line_sem):
    for i in range(rows.shape[0] // heads):
        pltpu.make_async_copy(
            rows.at[pl.ds(i * heads, heads), :], start_out.at[:, pl.ds(i * LANES, LANES)], line_sem
        ).start()
    copies = [
        pltpu.make_async_copy(x, y, sems.at[i])
        for i, (x, y) in enumerate(((gq, gq_out), (gk, gk_out), (gv, gv_out)))
    ]
    for copy in copies:
        copy.start()
    for copy in copies:
        copy.wait()
    pltpu.make_async_copy(rows, rows, line_sem).wait()


def per_device(queries, memory_keys, memory_values, upstream, inner_rate, checkpoints):
    heads = inner_rate.shape[1]
    features = queries.shape[2]
    dh = features // heads
    tokens = queries.shape[1]
    half = features // 2
    unit = min(4 * LANES, half)
    pieces = half // (2 * LANES)
    count = tokens // MB

    vmem = pl.BlockSpec(memory_space=pltpu.VMEM)
    hbm = pl.BlockSpec(memory_space=pl.ANY)
    kept = pl.BlockSpec(memory_space=pltpu.HBM)
    assert 2 * dh == LANES
    lines = dh * dh // LANES
    tall = jax.ShapeDtypeStruct((tokens, features), BF16)
    held = pltpu.VMEM((tokens, features), BF16)
    whole = pltpu.VMEM((dh, features), F32)
    part = pltpu.VMEM((dh, half), F32)
    rows = pltpu.VMEM((tokens, features), F32)
    gq, gk, gv, start_rows = pl.pallas_call(
        partial(kernel, dh, unit),
        in_specs=[kept] * 4 + [pl.BlockSpec(memory_space=pltpu.SMEM), kept],
        out_specs=[vmem] * 4,
        out_shape=[held, held, held, pltpu.VMEM((lines * heads, LANES), F32)],
        scratch_shapes=[held, held, held, pltpu.SemaphoreType.DMA((3,))] + [
            pltpu.VMEM((features // LANES * dh, LANES), F32),
            held,
            pltpu.VMEM((tokens, half), BF16),
            pltpu.VMEM((count * dh, features), F32),
            rows, rows, rows,
            whole,
            part, part, part, part, part, part,
            part, part, part,
            whole,
            pltpu.SemaphoreType.DMA,
            pltpu.SemaphoreType.DMA, pltpu.SemaphoreType.DMA((2 * pieces,)),
        ] + [pltpu.SemaphoreType.DMA, pltpu.SemaphoreType.DMA((pieces,))] * 2
        + [pltpu.SemaphoreType.DMA, pltpu.SemaphoreType.DMA((half // LANES,))] * 2,
        compiler_params=pltpu.CompilerParams(collective_id=0, has_side_effects=True, vmem_limit_bytes=61 * 2**20 + 2**19),
        name="layer_backward",
    )(upstream[0], queries[0], memory_keys[0], memory_values[0], inner_rate, checkpoints[0, 0])
    gq, gk, gv, start = pl.pallas_call(
        partial(store_kernel, heads),
        in_specs=[hbm] * 4,
        out_specs=[hbm] * 4,
        out_shape=[tall, tall, tall, jax.ShapeDtypeStruct((heads, dh * dh), F32)],
        scratch_shapes=[pltpu.SemaphoreType.DMA((3,)), pltpu.SemaphoreType.DMA],
        compiler_params=pltpu.CompilerParams(vmem_limit_bytes=2**20),
        name="store_results",
    )(gq, gk, gv, start_rows)
    return gq[None], gk[None], gv[None], start[None, None]


def solution(mesh):
    return jax.shard_map(
        per_device,
        mesh=mesh,
        in_specs=(
            P("section", "seq", None),
            P("section", "seq", None),
            P("section", "seq", None),
            P("section", "seq", None),
            P("section", None),
            P("section", "seq", None, None),
        ),
        out_specs=(
            P("section", "seq", None),
            P("section", "seq", None),
            P("section", "seq", None),
            P("section", "seq", None, None),
        ),
        check_vma=False,
    )
```

```python
from functools import partial

import jax
import jax.numpy as jnp
from jax import lax
from jax.experimental import pallas as pl
from jax.experimental.pallas import tpu as pltpu
from jax.sharding import PartitionSpec as P

MB = 64
LANES = 128
F32 = jnp.float32
BF16 = jnp.bfloat16
MESH = pl.DeviceIdType.MESH


def nn(a, b):
    return lax.dot_general(a, b, (((1,), (0,)), ((), ())), preferred_element_type=F32)


def nt(a, b):
    return lax.dot_general(a, b, (((1,), (1,)), ((), ())), preferred_element_type=F32)


def tn(a, b):
    return lax.dot_general(a, b, (((0,), (0,)), ((), ())), preferred_element_type=F32)


def split(x):
    high = x.astype(BF16)
    return high, (x - high.astype(F32)).astype(BF16)


def stacked(parts):
    return jnp.concatenate(parts, axis=0)


def tiles(x):
    return [x[:, i : i + LANES] for i in range(0, x.shape[1], LANES)]


def diagonal(x, dh):
    per = LANES // dh
    lane = lax.broadcasted_iota(jnp.int32, (x.shape[0], LANES), 1) // dh
    masks = [(lane == i).astype(F32).astype(BF16) for i in range(per)]
    pieces = tiles(x)
    zero = jnp.zeros((x.shape[0], LANES), x.dtype)
    rows = []
    for t, piece in enumerate(pieces):
        for i in range(per):
            row = [zero] * len(pieces)
            row[t] = piece * masks[i]
            rows.append(jnp.concatenate(row, axis=1))
    return stacked(rows)


def folded(a, b, dh):
    per = LANES // dh
    lane = lax.broadcasted_iota(jnp.int32, (dh, LANES), 1) // dh
    out = []
    for left, right in zip(tiles(a), tiles(b)):
        product = tn(left, right)
        value = product[:dh]
        for i in range(1, per):
            value = jnp.where(lane == i, product[i * dh : (i + 1) * dh], value)
        out.append(value)
    return jnp.concatenate(out, axis=1)


def rows_times(x, weights, multiply=nn):
    high, low = split(x)
    both = multiply(stacked([high, low]), weights)
    return both[: x.shape[0]] + both[x.shape[0] :]


def full_times(x, weights, multiply=nn):
    return rows_times(x, weights[0], multiply) + multiply(x.astype(BF16), weights[1])


def halves(x, dh):
    high, low = split(x)
    return diagonal(high, dh), diagonal(low, dh)


def exact_times(x, weights, multiply=nn):
    return multiply(x, weights[0]) + multiply(x, weights[1])


def doubled(a, b):
    return stacked([a, a]), stacked(split(b))


def lane_index(shape, dh):
    return lax.broadcasted_iota(jnp.int32, shape, 1) % dh


def upper_mask(width):
    row = lax.broadcasted_iota(jnp.int32, (MB, width), 0)
    return (lane_index((MB, width), MB) >= row).astype(F32)


def weight_part(k, v, c, w, dh):
    weights, errors = [], []
    for t in range(len(k)):
        e = exact_times(k[t], halves(w, dh)) - v[t].astype(F32)
        yield
        weights.append(w)
        errors.append(e)
        if t + 1 < len(k):
            w = w - c * folded(*doubled(k[t], e), dh)
            yield
    return weights, errors


def linear_part(k, c, dh):
    width = c.shape[1]
    row = lax.broadcasted_iota(jnp.int32, (dh, width), 0)
    eye = jnp.where(row == lane_index((dh, width), dh), 1.0, 0.0)
    linear = []
    for block in k:
        linear.append(eye - c * folded(block, block, dh))
        yield
    a = linear[-1]
    for t in range(len(k) - 2, -1, -1):
        a = full_times(linear[t], halves(a, dh))
        yield
    return a


def pair_linear(near, far, is_even, c, dh):
    near_a = yield from linear_part(near, c, dh)
    far_a = yield from linear_part(far, c, dh)
    first = jnp.where(is_even, near_a, far_a)
    second = jnp.where(is_even, far_a, near_a)
    both = full_times(first, halves(second, dh))
    yield
    return first, second, both


def interleaved(runs):
    results, waiting = [None] * len(runs), dict(enumerate(runs))
    while waiting:
        for i, run in list(waiting.items()):
            try:
                next(run)
            except StopIteration as stop:
                results[i] = stop.value
                del waiting[i]
    return results


def step_back(q, k, z, error_grad, dh):
    high, low = split(error_grad)
    return folded(stacked([q, k, k]), stacked([z, high, low]), dh)


def source_part(q, k, z, c, dh):
    upper = upper_mask(c.shape[1])
    carried = [None] * len(k)
    for t in range(len(k) - 1, -1, -1):
        scores = nt(k[t], diagonal(q[t], dh)) * upper
        yield
        carried[t] = rows_times(scores, diagonal(z[t], dh))
        yield
    b = None
    for t in range(len(k) - 1, -1, -1):
        total = carried[t] if b is None else carried[t] + exact_times(k[t], halves(b, dh))
        yield
        update = step_back(q[t], k[t], z[t], total * -c, dh)
        b = update if b is None else b + update
        yield
    return carried, b


def score_part(q, k, z, c, weights, errors, dh):
    upper = upper_mask(c.shape[1])
    query_grads, key_part = [], []
    for t in range(len(k)):
        score_grad = rows_times(errors[t], diagonal(z[t], dh), nt) * (upper * -c)
        yield
        key_part.append(rows_times(score_grad, diagonal(q[t], dh)))
        yield
        high, low = split(score_grad)
        query_grads.append(
            exact_times(z[t], halves(weights[t], dh), nt)
            + folded(stacked([high, low]), stacked([k[t], k[t]]), dh)
        )
        yield
    return query_grads, key_part


def final_part(q, k, z, c, weights, errors, carried, key_part, g, dh):
    count = len(q)
    key_grads, value_grads = [None] * count, [None] * count
    for t in range(count - 1, -1, -1):
        whole = halves(g, dh)
        minus = c * (carried[t] + exact_times(k[t], whole))
        yield
        value_grads[t] = minus
        g = g + step_back(q[t], k[t], z[t], -minus, dh)
        yield
        partial_grad = key_part[t] - c * full_times(errors[t], whole, nt)
        yield
        key_grads[t] = partial_grad - full_times(minus, halves(weights[t], dh), nt)
        yield
    return key_grads, value_grads, g


def cut(ref, lanes, size=MB):
    return [ref[i : i + size, lanes] for i in range(0, ref.shape[0], size)]


def put(ref, lanes, parts):
    size = ref.shape[0] // len(parts)
    for i, part in enumerate(parts):
        ref[i * size : (i + 1) * size, lanes] = part.astype(ref.dtype)


def kernel(
    dh, unit, upstream, q_in, k_in, v_in, rates, checkpoint,
    gq, gk, gv, rows_of_heads,
    q, k, v, in_sems, stage,
    z, far_k, trail, err, car, kp, b, other_b, first_a, second_a, pair_a, pair_b, second_b,
    entering, leaving, back, end,
    line_sem, up_send, up_recv, k_send, k_recv, b_send, b_recv, g_send, g_recv, r_send, r_recv,
):
    shard, shards = lax.axis_index("seq"), lax.axis_size("seq")
    section, sections = lax.axis_index("section"), lax.axis_size("section")
    features = q.shape[1]
    half = features // 2
    units = half // unit
    piece = 2 * LANES
    pieces = half // piece
    per_unit = unit // piece
    fine = piece // LANES
    side = lax.rem(shard, 2)
    is_even = side == 0
    partner = (section, shard + 1 - 2 * side)
    before = (section, jnp.maximum(shard - 2, 0))
    after = (section, jnp.minimum(shard + 2, shards - 1))
    below = (lax.rem(section + sections - 1, sections), shard)
    above = (lax.rem(section + 1, sections), shard)
    not_first = shard >= 2
    not_last = shard < shards - 2
    heads = features // dh
    lines = dh * dh // LANES

    def line_in(i):
        return pltpu.make_async_copy(
            checkpoint.at[:, pl.ds(i * LANES, LANES)],
            rows_of_heads.at[pl.ds(i * heads, heads), :],
            line_sem,
        )

    loads = [
        pltpu.make_async_copy(x, y, in_sems.at[i])
        for i, (x, y) in enumerate(((k_in, k), (v_in, v), (q_in, q)))
    ]
    loads[0].start()
    for i in range(lines):
        line_in(i).start()
    loads[1].start()
    loads[2].start()

    barrier = pltpu.get_barrier_semaphore()
    for peer in (below, above, partner):
        pl.semaphore_signal(barrier, inc=1, device_id=peer, device_id_type=MESH)
    for present, peer in ((not_first, before), (not_last, after)):
        @pl.when(present)
        def _():
            pl.semaphore_signal(barrier, inc=1, device_id=peer, device_id_type=MESH)

    def remote(source, target, send, recv, peer):
        return pltpu.make_async_remote_copy(
            src_ref=source, dst_ref=target, send_sem=send, recv_sem=recv,
            device_id=peer, device_id_type=MESH,
        )

    left = lax.broadcasted_iota(jnp.int32, (lines, LANES), 1) < dh

    def swap(x):
        return jnp.concatenate([x[:, dh:], x[:, :dh]], axis=1)

    def head_of(lanes):
        return (lanes.start // LANES) * (LANES // dh)

    def rate_of(lanes):
        head = head_of(lanes)
        first = lax.broadcasted_iota(jnp.int32, (1, LANES), 1) < dh
        return jnp.where(first, rates[0, head], rates[0, head + 1]) / MB

    def load_weight(lanes):
        head = head_of(lanes)
        x = rows_of_heads[pl.ds(head, lines, stride=heads), :]
        y = rows_of_heads[pl.ds(head + 1, lines, stride=heads), :]
        base = head * (dh // 2)
        stage[pl.ds(base, lines, stride=2), :] = jnp.where(left, x, swap(y))
        stage[pl.ds(base + 1, lines, stride=2), :] = jnp.where(left, swap(x), y)
        trail[:dh, lanes] = stage[pl.ds(pl.multiple_of(base, dh), dh), :]

    def store_start(lanes, first):
        head = head_of(lanes)
        base = head * (dh // 2)
        stage[pl.ds(pl.multiple_of(base, dh), dh), :] = first
        even = stage[pl.ds(base, lines, stride=2), :]
        odd = stage[pl.ds(base + 1, lines, stride=2), :]
        rows_of_heads[pl.ds(head, lines, stride=heads), :] = jnp.where(left, even, swap(odd))
        rows_of_heads[pl.ds(head + 1, lines, stride=heads), :] = jnp.where(left, swap(even), odd)

    def span(start, size):
        return pl.ds(pl.multiple_of(start, size), size)

    def own(i, size):
        return span(side * half + i * size, size)

    def others(i, size):
        return span((1 - side) * half + i * size, size)

    def place(i, size):
        return span(i * size, size)

    def source_lanes(i):
        return span(lax.rem(1 - side + i // units, 2) * half + lax.rem(i, units) * unit, unit)

    def send_up(i):
        start = source_lanes(i // per_unit).start + lax.rem(i, per_unit) * piece
        lanes = span(start, piece)
        return remote(upstream.at[:, lanes], z.at[:, lanes], up_send, up_recv.at[i], below)

    def send_k(i):
        return remote(
            k_in.at[:, others(i, piece)], far_k.at[:, place(i, piece)], k_send, k_recv.at[i], partner
        )

    def send_b(i):
        return remote(
            b.at[:, others(i, piece)], other_b.at[:, place(i, piece)], b_send, b_recv.at[i], partner
        )

    def send_g(i):
        return remote(
            leaving.at[:, place(i, LANES)], entering.at[:, place(i, LANES)], g_send, g_recv.at[i], before
        )

    def send_r(i, source):
        return remote(
            source.at[:, place(i, LANES)], end.at[:, own(i, LANES)], r_send, r_recv.at[i], partner
        )

    def await_r(i):
        return remote(
            back.at[:, place(i, LANES)], end.at[:, others(i, LANES)], r_send, r_recv.at[i], partner
        )

    sends_k = not_last | is_even
    gets_k = not_last | jnp.logical_not(is_even)
    sends_back = not_last | jnp.logical_not(is_even)
    gets_back = not_last | is_even

    def narrow(lanes):
        return [
            pl.ds(pl.multiple_of(lanes.start + j, LANES), LANES) for j in range(0, lanes.size, LANES)
        ]

    def together(compute, store, lanes):
        groups = narrow(lanes)
        results = interleaved([compute(x) for x in groups])
        for x, result in zip(groups, results):
            store(x, *result)

    def weights_of(lanes):
        return weight_part(cut(k, lanes), cut(v, lanes), rate_of(lanes), trail[:dh, lanes], dh)

    def put_weights(lanes, weights, errors):
        for t in range(1, len(weights)):
            trail[t * dh : (t + 1) * dh, lanes] = weights[t]
        put(err, lanes, errors)

    def sources_of(lanes):
        return source_part(cut(q, lanes), cut(k, lanes), cut(z, lanes), rate_of(lanes), dh)

    def put_sources(lanes, carried, offset):
        put(car, lanes, carried)
        b[:, lanes] = offset

    def scores_of(lanes):
        return score_part(
            cut(q, lanes), cut(k, lanes), cut(z, lanes), rate_of(lanes),
            cut(trail, lanes, dh), cut(err, lanes), dh,
        )

    def put_scores(lanes, query_grads, key_part):
        put(gq, lanes, query_grads)
        put(kp, lanes, key_part)

    def finals_of(lanes):
        return final_part(
            cut(q, lanes), cut(k, lanes), cut(z, lanes), rate_of(lanes),
            cut(trail, lanes, dh), cut(err, lanes), cut(car, lanes), cut(kp, lanes), end[:, lanes], dh,
        )

    def put_finals(lanes, key_grads, value_grads, first):
        put(gk, lanes, key_grads)
        put(gv, lanes, value_grads)
        store_start(lanes, first)

    def each(body, first, last):
        def step(i, nothing):
            body(i)
            return nothing

        lax.fori_loop(first, last, step, jnp.int32(0))

    def weight_step(i):
        lanes = span(i * unit, unit)
        for x in narrow(lanes):
            load_weight(x)
        together(weights_of, put_weights, lanes)

    def linear_step(i):
        @pl.when(gets_k)
        def _():
            for j in range(per_unit):
                send_k(i * per_unit + j).wait_recv()

        lanes = own(i, unit)
        offset = side * half

        def compute(x):
            local = pl.ds(pl.multiple_of(x.start - offset, LANES), LANES)
            return pair_linear(cut(k, x), cut(far_k, local), is_even, rate_of(x), dh)

        def store(x, first, second, both):
            local = pl.ds(pl.multiple_of(x.start - offset, LANES), LANES)
            first_a[:, local] = first
            second_a[:, local] = second
            pair_a[:, local] = both

        together(compute, store, lanes)

    def source_step(i):
        for j in range(per_unit):
            send_up(i * per_unit + j).wait_recv()
        together(sources_of, put_sources, source_lanes(i))

    def pair_step(i):
        lanes, local = own(i, piece), place(i, piece)
        send_b(i).wait_recv()
        near_b, far_b = b[:, lanes], other_b[:, local]
        b1 = jnp.where(is_even, far_b, near_b)
        b0 = jnp.where(is_even, near_b, far_b)
        offset = full_times(first_a[:, local], halves(b1, dh)) + b0
        pair_b[:, local] = offset
        second_b[:, local] = b1

        @pl.when(not_first & jnp.logical_not(not_last))
        def _():
            leaving[:, local] = offset
            for j in range(fine):
                send_g(i * fine + j).start()

    def relay_step(i):
        lanes, local = own(i, LANES), place(i, LANES)

        @pl.when(not_last)
        def _():
            send_g(i).wait_recv()

            @pl.when(is_even)
            def _():
                send_r(i, entering).start()

            incoming = entering[:, local]
            whole = halves(incoming, dh)

            @pl.when(not_first)
            def _():
                leaving[:, local] = full_times(pair_a[:, local], whole) + pair_b[:, local]
                send_g(i).start()

            middle = full_times(second_a[:, local], whole) + second_b[:, local]
            end[:, lanes] = jnp.where(is_even, middle, incoming)

            @pl.when(jnp.logical_not(is_even))
            def _():
                back[:, local] = middle
                send_r(i, back).start()

        @pl.when(jnp.logical_not(not_last))
        def _():
            middle = second_b[:, local]
            nothing = jnp.zeros_like(middle)
            end[:, lanes] = jnp.where(is_even, middle, nothing)

            @pl.when(jnp.logical_not(is_even))
            def _():
                back[:, local] = middle
                end[:, others(i, LANES)] = nothing
                send_r(i, back).start()

    def lanes_of(i):
        return span(lax.rem(side + i // units, 2) * half + lax.rem(i, units) * unit, unit)

    def score_step(i):
        together(scores_of, put_scores, lanes_of(i))

    def last_step(i):
        @pl.when((i >= units) & gets_back)
        def _():
            for j in range(unit // LANES):
                await_r((i - units) * (unit // LANES) + j).wait_recv()

        together(finals_of, put_finals, lanes_of(i))

    pl.semaphore_wait(barrier, 3 + not_first.astype(jnp.int32) + not_last.astype(jnp.int32))
    for i in range(2 * pieces):
        send_up(i).start()

    @pl.when(sends_k)
    def _():
        for i in range(pieces):
            send_k(i).start()

    pltpu.make_async_copy(rows_of_heads, rows_of_heads, line_sem).wait()
    loads[0].wait()
    loads[1].wait()
    total = 2 * units
    loads[2].wait()
    prepared = jnp.where(lax.rem(section, 2) == 0, total // 2, total)
    each(weight_step, 0, prepared)

    distance = (shards - 1 - shard) // 2
    near = distance == 1
    ahead = pieces // 2 * fine
    links = pieces * fine

    def advance(n):
        source_step(n)

        @pl.when(n < units)
        def _():
            for j in range(per_unit):
                send_b(n * per_unit + j).start()

        each(weight_step, prepared, jnp.where(n == units - 1, total, prepared))

        @pl.when((n >= units - 1) & (n < total - 1))
        def _():
            linear_step(n - (units - 1))

        each(relay_step, 0, jnp.where((n == total - 1) & near, ahead, 0))

        @pl.when(n >= units)
        def _():
            for j in range(per_unit):
                pair_step((n - units) * per_unit + j)

    each(advance, 0, total)

    each(relay_step, ahead, jnp.where(near, links, ahead))

    relay_at = jnp.where(
        distance == 0, 0, jnp.where(near, -3, jnp.where(distance == 2, total - 1, total))
    )
    relay_from = jnp.where(near, pieces, 0)
    pause = jnp.where(distance == 2, total - 1, 2 * total)
    early = jnp.where(not_first | near, 0, 1)

    def slot(n):
        now = n - relay_at

        @pl.when((now >= relay_from) & (now < pieces))
        def _():
            for j in range(fine):
                relay_step(now * fine + j)

        chosen = n - (n > pause).astype(jnp.int32)

        @pl.when((chosen < total) & (n != pause))
        def _():
            score_step(chosen)

        index = jnp.where(now == 1, 0, now - 3 + early)

        @pl.when((index < total) & ((now >= 3) | ((now == 1) & (early == 1))))
        def _():
            last_step(index)

    each(slot, 0, relay_at + 3 + total)

    remote(upstream, z, up_send, up_recv.at[0], below).wait_send()
    remote(b.at[:, others(0, half)], other_b, b_send, b_recv.at[0], partner).wait_send()

    @pl.when(sends_k)
    def _():
        remote(k_in.at[:, others(0, half)], far_k, k_send, k_recv.at[0], partner).wait_send()

    @pl.when(sends_back)
    def _():
        remote(back, end.at[:, own(0, half)], r_send, r_recv.at[0], partner).wait_send()

    @pl.when(not_first)
    def _():
        remote(leaving, entering, g_send, g_recv.at[0], before).wait_send()


def store_kernel(heads, gq, gk, gv, rows, gq_out, gk_out, gv_out, start_out, sems, line_sem):
    for i in range(rows.shape[0] // heads):
        pltpu.make_async_copy(
            rows.at[pl.ds(i * heads, heads), :], start_out.at[:, pl.ds(i * LANES, LANES)], line_sem
        ).start()
    copies = [
        pltpu.make_async_copy(x, y, sems.at[i])
        for i, (x, y) in enumerate(((gq, gq_out), (gk, gk_out), (gv, gv_out)))
    ]
    for copy in copies:
        copy.start()
    for copy in copies:
        copy.wait()
    pltpu.make_async_copy(rows, rows, line_sem).wait()


def per_device(queries, memory_keys, memory_values, upstream, inner_rate, checkpoints):
    heads = inner_rate.shape[1]
    features = queries.shape[2]
    dh = features // heads
    tokens = queries.shape[1]
    half = features // 2
    unit = min(4 * LANES, half)
    pieces = half // (2 * LANES)
    count = tokens // MB

    vmem = pl.BlockSpec(memory_space=pltpu.VMEM)
    hbm = pl.BlockSpec(memory_space=pl.ANY)
    kept = pl.BlockSpec(memory_space=pltpu.HBM)
    assert 2 * dh == LANES
    lines = dh * dh // LANES
    tall = jax.ShapeDtypeStruct((tokens, features), BF16)
    held = pltpu.VMEM((tokens, features), BF16)
    whole = pltpu.VMEM((dh, features), F32)
    part = pltpu.VMEM((dh, half), F32)
    rows = pltpu.VMEM((tokens, features), F32)
    gq, gk, gv, start_rows = pl.pallas_call(
        partial(kernel, dh, unit),
        in_specs=[kept] * 4 + [pl.BlockSpec(memory_space=pltpu.SMEM), kept],
        out_specs=[vmem] * 4,
        out_shape=[held, held, held, pltpu.VMEM((lines * heads, LANES), F32)],
        scratch_shapes=[held, held, held, pltpu.SemaphoreType.DMA((3,))] + [
            pltpu.VMEM((features // LANES * dh, LANES), F32),
            held,
            pltpu.VMEM((tokens, half), BF16),
            pltpu.VMEM((count * dh, features), F32),
            rows, rows, rows,
            whole,
            part, part, part, part, part, part,
            part, part, part,
            whole,
            pltpu.SemaphoreType.DMA,
            pltpu.SemaphoreType.DMA, pltpu.SemaphoreType.DMA((2 * pieces,)),
        ] + [pltpu.SemaphoreType.DMA, pltpu.SemaphoreType.DMA((pieces,))] * 2
        + [pltpu.SemaphoreType.DMA, pltpu.SemaphoreType.DMA((half // LANES,))] * 2,
        compiler_params=pltpu.CompilerParams(collective_id=0, has_side_effects=True, vmem_limit_bytes=61 * 2**20 + 2**19),
        name="layer_backward",
    )(upstream[0], queries[0], memory_keys[0], memory_values[0], inner_rate, checkpoints[0, 0])
    gq, gk, gv, start = pl.pallas_call(
        partial(store_kernel, heads),
        in_specs=[hbm] * 4,
        out_specs=[hbm] * 4,
        out_shape=[tall, tall, tall, jax.ShapeDtypeStruct((heads, dh * dh), F32)],
        scratch_shapes=[pltpu.SemaphoreType.DMA((3,)), pltpu.SemaphoreType.DMA],
        compiler_params=pltpu.CompilerParams(vmem_limit_bytes=2**20),
        name="store_results",
    )(gq, gk, gv, start_rows)
    return gq[None], gk[None], gv[None], start[None, None]


def solution(mesh):
    return jax.shard_map(
        per_device,
        mesh=mesh,
        in_specs=(
            P("section", "seq", None),
            P("section", "seq", None),
            P("section", "seq", None),
            P("section", "seq", None),
            P("section", None),
            P("section", "seq", None, None),
        ),
        out_specs=(
            P("section", "seq", None),
            P("section", "seq", None),
            P("section", "seq", None),
            P("section", "seq", None, None),
        ),
        check_vma=False,
    )
```
